32 devices in a mesh: row: 8 (over z, x), col: 4 (over y, core).
Axes of the slice: x: 2, y: 2, z: 4, core: 2. Of those that a mesh axis runs over, the one named last changes fastest.
Arguments:
- values: bfloat16 [8, 4, 2, 128, 128], P('row', 'col'), may hold values from -6 to 6
- occupancy: int32 [8, 4, 2], replicated, may hold values from 0 to 8, as said below
Outputs:
- square: bfloat16 [8, 4, 2, 128, 128], P('row', 'col')
- updated: float32 [8, 4, 2, 128, 128], P('row', 'col')
The draws below stay inside these ranges and needn't reach their ends.
Inputs may be any that keep to these rules, and one draw needn't show every extreme that they name: `occupancy`: within each tile the slots that are not 2 * 4 name distinct positions; a slot holding 2 * 4 is empty. Every tile has one or more stored blocks; in every draw some tile has all 2 slots stored and some tile has an empty slot.
All inputs are finite; a program needn't handle non-finite values.
Results may differ from the reference program's by a relative error of at most 0.0018.
Values may be sent and summed in bfloat16 or wider, within the bound.
No kernel may reach another device: no remote copies, remote signals or barrier semaphores. Data moves between devices by JAX's collectives and lax.ppermute only.
A program may use at most 64 MiB of HBM per device.

```python
import math
import jax
import jax.numpy as jnp
from jax import lax

BLOCK = 128
RB = 2
CB = 4
SLOTS = 2
TILE_ROWS = 8
TILE_COLS = 4
ORDER = 2048


def draw_occupancy(key, part):
    cells = TILE_ROWS * TILE_COLS
    positions = RB * CB
    base = jax.random.fold_in(key, 7)
    first_key, second_key, third_key, fourth_key = jax.random.split(base, 4)
    orders = jax.vmap(lambda single: jax.random.permutation(single, positions))(jax.random.split(first_key, cells))
    orders = orders[:, :SLOTS].astype(jnp.int32)
    counts = jax.random.randint(second_key, (cells,), 1, SLOTS + 1)
    chosen = jax.random.randint(third_key, (), 0, cells)
    sparse_cell = (chosen + jax.random.randint(fourth_key, (), 1, cells)) % cells
    cell_list = jnp.arange(cells)
    counts = jnp.where(cell_list == sparse_cell, 1, counts)
    counts = jnp.where(cell_list == chosen, SLOTS, counts)
    slot_index = jnp.arange(SLOTS)[None, :]
    result = jnp.where(slot_index < counts[:, None], orders, positions)
    return result.reshape(TILE_ROWS, TILE_COLS, SLOTS).astype(jnp.int32)


def levels(stream_key, dims, shards, low, high):
    factor_of, own = 1.0, jax.random.fold_in(stream_key, 6)
    for axis_at, parts in shards:
        heights = jnp.exp(jax.random.uniform(jax.random.fold_in(own, axis_at), (parts,), jnp.float32, low / len(shards), high / len(shards)))
        factor_of = factor_of * jnp.repeat(heights, dims[axis_at] // parts).reshape([-1 if axis == axis_at else 1 for axis in range(len(dims))])
    return factor_of


def bell_draw(own_key, shape, scale, bound, cuts=(), kind=jnp.bfloat16):
    loudness = levels(own_key, shape, cuts, -0.22, 0.18) if cuts else 1.0
    values = jax.random.normal(own_key, shape, jnp.float32) * scale * loudness
    return jnp.minimum(jnp.maximum(values, -bound), bound).astype(kind)


def setup_inputs(seed: int = 0) -> dict:
    splits = jax.random.split(jax.random.key(seed), 3)
    return {
        "values": bell_draw(splits[0], (TILE_ROWS, TILE_COLS, SLOTS, BLOCK, BLOCK), 1.0, 6.0, ((0, 8), (1, 4))),
        "occupancy": draw_occupancy(jax.random.fold_in(splits[2], 71), 0),
    }


def unpack(packed, occupancy):
    positions = jnp.arange(RB * CB, dtype=jnp.int32)
    onehot = (occupancy[:, :, None, :] == positions[None, None, :, None]).astype(jnp.float32)
    blocks = jnp.einsum('abps,absxy->abpxy', onehot, packed.astype(jnp.float32), precision=lax.Precision.HIGHEST)
    blocks = blocks.reshape(TILE_ROWS, TILE_COLS, RB, CB, BLOCK, BLOCK)
    return blocks.transpose(0, 2, 4, 1, 3, 5).reshape(ORDER, ORDER)

def restricted(left, right, occupancy):
    tile_row_list = jnp.repeat(jnp.arange(TILE_ROWS, dtype=jnp.int32), TILE_COLS)
    tile_col_list = jnp.tile(jnp.arange(TILE_COLS, dtype=jnp.int32), TILE_ROWS)
    flat = occupancy.reshape(TILE_ROWS * TILE_COLS, SLOTS).astype(jnp.int32)

    def one_tile(item):
        tile_row, tile_col, index = item
        clipped = jnp.minimum(index, RB * CB - 1)
        row_start = ((tile_row * RB + clipped // CB) * BLOCK).astype(jnp.int32)
        col_start = ((tile_col * CB + clipped % CB) * BLOCK).astype(jnp.int32)

        def one_slot(pair):
            first_row, first_col = pair
            rows = lax.dynamic_slice(left, (first_row, jnp.int32(0)), (BLOCK, ORDER))
            columns = lax.dynamic_slice(right, (jnp.int32(0), first_col), (ORDER, BLOCK))
            return jnp.dot(rows, columns, precision=lax.Precision.HIGHEST, preferred_element_type=jnp.float32)
        blocks = lax.map(one_slot, (row_start, col_start))
        live = (index < RB * CB).astype(jnp.float32)[:, None, None]
        return blocks * live
    result = lax.map(one_tile, (tile_row_list, tile_col_list, flat))
    return result.reshape(TILE_ROWS, TILE_COLS, SLOTS, BLOCK, BLOCK)

def reference(values, occupancy):
    live = (occupancy < RB * CB).astype(jnp.float32)[:, :, :, None, None]
    wide = unpack(values, occupancy)
    factor = 5.0 / math.sqrt(ORDER)
    square = (factor * restricted(wide, wide, occupancy)).astype(jnp.bfloat16)
    s_wide = unpack(square, occupancy)
    cube = restricted(s_wide, wide, occupancy)
    updated = 1.5 * (values.astype(jnp.float32) * live) - 0.5 * factor * cube
    return (square, updated)
```

```python
import functools
import math

import jax
import jax.numpy as jnp
from jax import lax
from jax.experimental import pallas as pl
from jax.experimental.pallas import tpu as pltpu
from jax.sharding import PartitionSpec as P

RB = 2


def flip(array, axis, size, offset):
    return lax.ppermute(array, axis, [(i, i ^ offset) for i in range(size)])


def column_tiles(own, size):
    inner = 2 if size % 2 == 0 else 1
    tiles = {0: own}
    outer = size // inner
    for far in reversed(range(2, outer)):
        tiles[far * inner] = flip(own, "row", size, far * inner)
    near = range(inner * min(outer, 2))
    for offset in reversed(near):
        if offset:
            tiles[offset] = flip(own, "row", size, offset)
    if inner == 2:
        for far in reversed(range(2, outer)):
            tiles[far * inner + 1] = flip(tiles[far * inner], "row", size, 1)
    return [tiles[offset] for offset in range(size)]


def row_tiles(own, size):
    return [own] + [flip(own, "col", size, offset) for offset in range(1, size)]


def match_pairs(occ, pairs, row, col, sizes):
    row_count, slots, tile_rows, tile_cols = sizes
    positions = tile_rows * tile_cols
    own = [occ[row, col, s] for s in range(slots)]
    counts = [jnp.int32(0)] * slots
    for offset in range(row_count):
        tile = row ^ offset
        for u in range(slots):
            q = occ[tile, col, u]
            inner = tile * tile_rows + q // tile_cols
            column = q % tile_cols
            panel = jnp.minimum(inner // tile_cols, occ.shape[1] - 1)
            for s in range(slots):
                wanted = own[s] // tile_cols * tile_cols + inner % tile_cols
                hits = [occ[row, panel, v] == wanted for v in range(slots)]
                place = jnp.int32(0)
                hit = hits[0]
                for v in range(1, slots):
                    place = jnp.where(hits[v], v, place)
                    hit = jnp.logical_or(hit, hits[v])
                take = hit & (q < positions) & (own[s] < positions) & (own[s] % tile_cols == column)
                pairs[s, 0, counts[s]] = panel * slots + place
                pairs[s, 1, counts[s]] = jnp.int32(offset * slots + u)
                counts[s] = counts[s] + take.astype(jnp.int32)
    return counts


def pair_sums(pairs, counts, left, right, slots, zero_block):
    most = functools.reduce(jnp.maximum, counts)

    def step(turn, totals):
        result = []
        for s in range(slots):
            lefts, rights = [], []
            for half in range(2):
                at = 2 * turn + half
                live = at < counts[s]
                lefts.append(left[jnp.where(live, pairs[s, 0, at], zero_block)])
                rights.append(right[jnp.where(live, pairs[s, 1, at], 0)])
            result.append(
                totals[s]
                + jnp.dot(
                    jnp.concatenate(lefts, axis=1),
                    jnp.concatenate(rights, axis=0),
                    preferred_element_type=jnp.float32,
                )
            )
        return tuple(result)

    block = right.shape[-1]
    zeros = tuple(jnp.zeros((block, block), jnp.float32) for _ in range(slots))
    return lax.fori_loop(0, (most + 1) // 2, step, zeros)


def square_kernel(sizes, factor, *refs):
    row_count, col_count, slots, tile_rows, tile_cols = sizes
    occ = refs[0]
    rights = refs[1 : 1 + row_count]
    lefts = refs[1 + row_count : row_count + col_count]
    out, left, right, pairs = refs[row_count + col_count :]
    row, col = lax.axis_index("row"), lax.axis_index("col")
    zero_block = col_count * slots
    for offset in range(row_count):
        right[offset * slots : (offset + 1) * slots] = rights[offset][...]
    left[pl.ds(col * slots, slots)] = rights[0][...]
    for offset in range(1, col_count):
        left[pl.ds((col ^ offset) * slots, slots)] = lefts[offset - 1][...]
    left[zero_block] = jnp.zeros(left.shape[1:], left.dtype)
    counts = match_pairs(occ, pairs, row, col, (row_count, slots, tile_rows, tile_cols))
    sums = pair_sums(pairs, counts, left, right, slots, zero_block)
    for s in range(slots):
        out[s] = (factor * sums[s]).astype(out.dtype)


def cube_kernel(sizes, factor, *refs):
    row_count, col_count, slots, tile_rows, tile_cols = sizes
    occ = refs[0]
    rights = refs[1 : 1 + row_count]
    gathered = refs[1 + row_count]
    out, left, right, pairs = refs[2 + row_count :]
    row, col = lax.axis_index("row"), lax.axis_index("col")
    zero_block = col_count * slots
    for offset in range(row_count):
        right[offset * slots : (offset + 1) * slots] = rights[offset][...]
    left[0:zero_block] = gathered[...]
    left[zero_block] = jnp.zeros(left.shape[1:], left.dtype)
    counts = match_pairs(occ, pairs, row, col, (row_count, slots, tile_rows, tile_cols))
    sums = pair_sums(pairs, counts, left, right, slots, zero_block)
    for s in range(slots):
        stored = (occ[row, col, s] < tile_rows * tile_cols).astype(jnp.float32)
        own = rights[0][s].astype(jnp.float32) * stored
        out[s] = 1.5 * own - (0.5 * factor) * sums[s]


def per_device(values, occupancy):
    row_count = lax.axis_size("row")
    col_count = lax.axis_size("col")
    slots = values.shape[2]
    block = values.shape[-1]
    tile_rows = RB
    tile_cols = RB * row_count // col_count
    factor = 5.0 / math.sqrt(tile_rows * block * row_count)
    sizes = (row_count, col_count, slots, tile_rows, tile_cols)
    own = values.reshape(slots, block, block)
    rights = column_tiles(own, row_count)
    lefts = row_tiles(own, col_count)
    vmem = pl.BlockSpec(memory_space=pltpu.VMEM)
    smem = pl.BlockSpec(memory_space=pltpu.SMEM)
    scratch = [
        pltpu.VMEM((col_count * slots + 1, block, block), jnp.bfloat16),
        pltpu.VMEM((row_count * slots, block, block), jnp.bfloat16),
        pltpu.SMEM((slots, 2, row_count * slots + 2), jnp.int32),
    ]
    limit = pltpu.CompilerParams(vmem_limit_bytes=24 * 1024 * 1024)
    square = pl.pallas_call(
        functools.partial(square_kernel, sizes, factor),
        out_shape=jax.ShapeDtypeStruct((slots, block, block), jnp.bfloat16),
        in_specs=[smem] + [vmem] * (row_count + col_count - 1),
        out_specs=vmem,
        scratch_shapes=scratch,
        compiler_params=limit,
    )(occupancy, *rights, *lefts[1:])
    gathered = lax.all_gather(square, "col", axis=0, tiled=True)
    updated = pl.pallas_call(
        functools.partial(cube_kernel, sizes, factor),
        out_shape=jax.ShapeDtypeStruct((slots, block, block), jnp.float32),
        in_specs=[smem] + [vmem] * (row_count + 1),
        out_specs=vmem,
        scratch_shapes=scratch,
        compiler_params=limit,
    )(occupancy, *rights, gathered)
    shape_out = (1, 1, slots, block, block)
    return (square.reshape(shape_out), updated.reshape(shape_out))


def solution(mesh):
    spec = P("row", "col", None, None, None)
    return jax.shard_map(
        per_device,
        mesh=mesh,
        in_specs=(spec, P()),
        out_specs=(spec, spec),
        check_vma=False,
    )
```

```python
import functools
import math

import jax
import jax.numpy as jnp
from jax import lax
from jax.experimental import pallas as pl
from jax.experimental.pallas import tpu as pltpu
from jax.sharding import PartitionSpec as P


RB = 2


def routes(row_count, col_count):
    inner = 2 if row_count % 2 == 0 else 1
    far = [inner * z for z in range(2, row_count // inner)]
    order = [(f"r{k}", "row", None, k) for k in reversed(far)]
    near = [k for k in (1, 3, 2) if k < row_count and k not in far]
    order += [(f"r{k}", "row", None, k) for k in near]
    half = [k for k in range(1, col_count) if k == 1 or k % 2 == 0]
    order += [(f"c{k}", "col", None, k) for k in half]
    if inner == 2:
        order += [(f"r{k + 1}", "row", f"r{k}", 1) for k in reversed(far)]
    order += [(f"c{k + 1}", "col", f"c{k}", 1) for k in half if k > 1]
    return order


def gather(own, row_count, col_count):
    sizes = {"row": row_count, "col": col_count}
    held = {}
    for name, axis, source, offset in routes(row_count, col_count):
        held[name] = lax.ppermute(
            own if source is None else held[source],
            axis,
            [(i, i ^ offset) for i in range(sizes[axis])],
        )
    rights = [held[f"r{k}"] for k in range(1, row_count)]
    lefts = [held[f"c{k}"] for k in range(1, col_count)]
    return rights, lefts


def regather(square, col_count):
    held = {}
    for name, axis, source, offset in routes(1, col_count):
        held[name] = lax.ppermute(
            square if source is None else held[source],
            axis,
            [(i, i ^ offset) for i in range(col_count)],
        )
    return [held[f"c{k}"] for k in range(1, col_count)]


def split(number, divisor):
    if divisor & (divisor - 1) == 0:
        return number >> (divisor.bit_length() - 1), number & (divisor - 1)
    return lax.div(number, divisor), lax.rem(number, divisor)


def stage_kernel(values, own):
    own[...] = values[...]


def plan_kernel(sizes, occ, plan):
    row_count, col_count, slots, tile_rows, tile_cols, room = sizes
    row, col = lax.axis_index("row"), lax.axis_index("col")
    positions = tile_rows * tile_cols
    mine = [occ[col, s, row] for s in range(slots)]
    lines = [split(q, tile_cols) for q in mine]
    lines = [(line * tile_cols, jnp.where(q < positions, c, -1)) for q, (line, c) in zip(mine, lines)]
    ends = [jnp.int32(s * room + 1) for s in range(slots)]
    for offset in range(row_count):
        tile = row ^ offset
        for u in range(slots):
            q = occ[col, u, tile]
            line, column = split(q, tile_cols)
            panel, depth = split(tile * tile_rows + jnp.minimum(line, tile_rows - 1), tile_cols)
            column = jnp.where(q < positions, column, -2)
            base = (panel ^ col) * slots
            held = [occ[panel, v, row] for v in range(slots)]
            for s in range(slots):
                wanted = jnp.where(lines[s][1] == column, lines[s][0] + depth, -1)
                place = base
                hit = held[0] == wanted
                for v in range(1, slots):
                    also = held[v] == wanted
                    place = jnp.where(also, base + v, place)
                    hit = hit | also
                plan[ends[s]] = place
                plan[ends[s] + 1] = jnp.int32(offset * slots + u)
                ends[s] = ends[s] + jnp.where(hit, 2, 0)
    for s in range(slots):
        plan[s * room] = (ends[s] - (s * room + 1)) >> 1
        plan[(s + 1) * room - 1] = (mine[s] < positions).astype(jnp.int32)
        plan[ends[s]] = jnp.int32(col_count * slots)
        plan[ends[s] + 1] = jnp.int32(0)


def pair_sums(plan, room, left, right, slots):
    counts = [plan[s * room] for s in range(slots)]
    most = functools.reduce(jnp.maximum, counts)
    zero_block = left.shape[0] - 1

    def step(turn, totals):
        result = []
        for s in range(slots):
            lefts, rights = [], []
            for half in range(2):
                at = 2 * turn + half
                live = at < counts[s]
                at = s * room + 1 + 2 * jnp.minimum(at, counts[s])
                lefts.append(left[jnp.where(live, plan[at], zero_block)])
                rights.append(right[plan[at + 1]])
            product = jnp.dot(
                jnp.concatenate(lefts, axis=1),
                jnp.concatenate(rights, axis=0),
                preferred_element_type=jnp.float32,
            )
            result.append(totals[s] + product)
        return tuple(result)

    block = right.shape[-1]
    zeros = tuple(jnp.zeros((block, block), jnp.float32) for _ in range(slots))
    return lax.fori_loop(0, (most + 1) // 2, step, zeros)


def stack(target, tiles, slots):
    for at, tile in enumerate(tiles):
        target[at * slots : (at + 1) * slots] = tile[...]


def square_kernel(sizes, factor, *refs):
    row_count, col_count, slots, _, _, room = sizes
    plan_in = refs[0]
    rights = refs[1 : 1 + row_count]
    lefts = refs[1 + row_count : row_count + col_count]
    out, left, right, plan, sem = refs[row_count + col_count :]
    copy = pltpu.make_async_copy(plan_in, plan, sem)
    copy.start()
    stack(right, rights, slots)
    stack(left, (rights[0],) + lefts, slots)
    left[col_count * slots] = jnp.zeros(left.shape[1:], left.dtype)
    copy.wait()
    sums = pair_sums(plan, room, left, right, slots)
    for s in range(slots):
        out[s] = (factor * sums[s]).astype(out.dtype)


def cube_kernel(sizes, factor, *refs):
    row_count, col_count, slots, _, _, room = sizes
    plan_in = refs[0]
    rights = refs[1 : 1 + row_count]
    lefts = refs[1 + row_count : 1 + row_count + col_count]
    square, updated, left, right, result, plan, sem, square_sem, out_sem = refs[1 + row_count + col_count :]
    square_copy = pltpu.make_async_copy(lefts[0], square, square_sem)
    square_copy.start()
    copy = pltpu.make_async_copy(plan_in, plan, sem)
    copy.start()
    stack(right, rights, slots)
    stack(left, lefts, slots)
    left[col_count * slots] = jnp.zeros(left.shape[1:], left.dtype)
    copy.wait()
    sums = pair_sums(plan, room, left, right, slots)
    copies = []
    for s in range(slots):
        stored = plan[(s + 1) * room - 1].astype(jnp.float32)
        own = rights[0][s].astype(jnp.float32) * stored
        result[s] = 1.5 * own - (0.5 * factor) * sums[s]
        copies.append(pltpu.make_async_copy(result.at[s], updated.at[s], out_sem.at[s]))
        copies[-1].start()
    for done in copies:
        done.wait()
    square_copy.wait()


def per_device(values, occupancy):
    row_count = lax.axis_size("row")
    col_count = lax.axis_size("col")
    slots = values.shape[2]
    block = values.shape[-1]
    tile_rows = RB
    tile_cols = RB * row_count // col_count
    factor = 5.0 / math.sqrt(tile_rows * block * row_count)
    room = 2 * (row_count * slots + 1) + 2
    sizes = (row_count, col_count, slots, tile_rows, tile_cols, room)
    values = values.reshape(slots, block, block)
    vmem = pl.BlockSpec(memory_space=pltpu.VMEM)
    smem = pl.BlockSpec(memory_space=pltpu.SMEM)
    anywhere = pl.BlockSpec(memory_space=pl.ANY)
    limit = pltpu.CompilerParams(vmem_limit_bytes=24 * 1024 * 1024)
    tile = jax.ShapeDtypeStruct((slots, block, block), jnp.bfloat16)
    dma = pltpu.SemaphoreType.DMA
    scratch = [
        pltpu.VMEM((col_count * slots + 1, block, block), jnp.bfloat16),
        pltpu.VMEM((row_count * slots, block, block), jnp.bfloat16),
    ]
    own = pl.pallas_call(
        stage_kernel,
        out_shape=tile,
        in_specs=[vmem],
        out_specs=vmem,
        compiler_params=limit,
        name="stage",
    )(values)
    rights, lefts = gather(own, row_count, col_count)
    plan = pl.pallas_call(
        functools.partial(plan_kernel, sizes),
        out_shape=jax.ShapeDtypeStruct((slots * room,), jnp.int32),
        in_specs=[smem],
        out_specs=smem,
        compiler_params=limit,
        name="plan",
    )(occupancy.transpose(1, 2, 0))
    square = pl.pallas_call(
        functools.partial(square_kernel, sizes, factor),
        out_shape=tile,
        in_specs=[anywhere] + [vmem] * (row_count + col_count - 1),
        out_specs=vmem,
        scratch_shapes=scratch + [pltpu.SMEM((slots * room,), jnp.int32), dma],
        compiler_params=limit,
        name="square",
    )(plan, own, *rights, *lefts)
    others = regather(square, col_count)
    square_out, updated = pl.pallas_call(
        functools.partial(cube_kernel, sizes, factor),
        out_shape=(tile, jax.ShapeDtypeStruct((slots, block, block), jnp.float32)),
        in_specs=[anywhere] + [vmem] * (row_count + col_count),
        out_specs=(anywhere, anywhere),
        scratch_shapes=scratch
        + [
            pltpu.VMEM((slots, block, block), jnp.float32),
            pltpu.SMEM((slots * room,), jnp.int32),
            dma,
            dma,
            dma((slots,)),
        ],
        compiler_params=limit,
        name="cube",
    )(plan, own, *rights, square, *others)
    shape_out = (1, 1, slots, block, block)
    return (square_out.reshape(shape_out), updated.reshape(shape_out))


def solution(mesh):
    spec = P("row", "col", None, None, None)

    return jax.shard_map(
        per_device,
        mesh=mesh,
        in_specs=(spec, P()),
        out_specs=(spec, spec),
        check_vma=False,
    )
```

```python
import functools
import math

import jax
import jax.numpy as jnp
from jax import lax
from jax.experimental import pallas as pl
from jax.experimental.pallas import tpu as pltpu
from jax.sharding import PartitionSpec as P


RB = 2
PARAMS = pltpu.CompilerParams(vmem_limit_bytes=24 * 1024 * 1024)
VMEM = pl.BlockSpec(memory_space=pltpu.VMEM)
SMEM = pl.BlockSpec(memory_space=pltpu.SMEM)
ANY = pl.BlockSpec(memory_space=pl.ANY)


def send(array, axis, offset):
    size = lax.axis_size(axis)
    return lax.ppermute(array, axis, [(i, i ^ offset) for i in range(size)])


def join_kernel(*refs):
    at = 0
    for ref in refs[:-1]:
        refs[-1][at : at + ref.shape[0]] = ref[...]
        at += ref.shape[0]


def join(*arrays):
    shape = (sum(a.shape[0] for a in arrays),) + arrays[0].shape[1:]
    return pl.pallas_call(
        join_kernel,
        out_shape=jax.ShapeDtypeStruct(shape, arrays[0].dtype),
        in_specs=[VMEM] * len(arrays),
        out_specs=VMEM,
        compiler_params=PARAMS,
        name="join",
    )(*arrays)


def far_rows(row_count):
    return list(range(row_count - 2, 2, -2))


def column_order(row_count):
    far = far_rows(row_count)
    early = [0] + far + [2, 1]
    late = [3] + [k + 1 for k in far]
    return early, late


def gather(own, row_count, col_count):
    far = far_rows(row_count)
    rows = {k: send(own, "row", k) for k in far + [2]}
    near = send(own, "col", 1)
    rows[1] = send(own, "row", 1)
    pair = join(own, near)
    lefts = [near] + [send(pair, "col", k) for k in range(2, col_count, 2)]
    late = [send(join(rows[2], rows[far[0]]), "row", 1)]
    late += [send(rows[k], "row", 1) for k in far[1:]]
    return [rows[k] for k in far + [2, 1]], late, lefts


def split(number, divisor):
    if divisor & (divisor - 1) == 0:
        return number >> (divisor.bit_length() - 1), number & (divisor - 1)
    return lax.div(number, divisor), lax.rem(number, divisor)


def make_plan(sizes, occ, plan):
    row_count, _, slots, tile_rows, tile_cols, room = sizes
    row, col = lax.axis_index("row"), lax.axis_index("col")
    positions = tile_rows * tile_cols
    mine = [occ[col, s, row] for s in range(slots)]
    lines = [split(q, tile_cols) for q in mine]
    lines = [(line * tile_cols, jnp.where(q < positions, c, -1)) for q, (line, c) in zip(mine, lines)]
    ends = [jnp.int32(s * room + 1) for s in range(slots)]
    early, late = column_order(row_count)
    for at, offset in enumerate(early + late):
        tile = row ^ offset
        for u in range(slots):
            q = occ[col, u, tile]
            line, column = split(q, tile_cols)
            panel, depth = split(tile * tile_rows + jnp.minimum(line, tile_rows - 1), tile_cols)
            column = jnp.where(q < positions, column, -2)
            base = (panel ^ col) * slots
            held = [occ[panel, v, row] for v in range(slots)]
            for s in range(slots):
                wanted = jnp.where(lines[s][1] == column, lines[s][0] + depth, -1)
                place = base
                hit = held[0] == wanted
                for v in range(1, slots):
                    also = held[v] == wanted
                    place = jnp.where(also, base + v, place)
                    hit = hit | also
                plan[ends[s]] = place
                plan[ends[s] + 1] = jnp.int32(at * slots + u)
                ends[s] = ends[s] + jnp.where(hit, 2, 0)
    for s in range(slots):
        plan[s * room] = (ends[s] - (s * room + 1)) >> 1
        plan[(s + 1) * room - 1] = (mine[s] < positions).astype(jnp.int32)
        plan[ends[s]] = jnp.int32(0)
        plan[ends[s] + 1] = jnp.int32(0)


def pair_sums(plan, room, left, right, slots):
    counts = [plan[s * room] for s in range(slots)]
    most = functools.reduce(jnp.maximum, counts)
    zero_block = left.shape[0] - 1
    last = right.shape[0] - 1

    def step(turn, totals):
        result = []
        for s in range(slots):
            lefts, rights = [], []
            for half in range(2):
                at = 2 * turn + half
                live = at < counts[s]
                at = s * room + 1 + 2 * jnp.minimum(at, counts[s])
                place, other = plan[at], plan[at + 1]
                live = live & (place < zero_block) & (other <= last)
                lefts.append(left[jnp.where(live, place, zero_block)])
                rights.append(right[jnp.minimum(other, last)])
            product = jnp.dot(
                jnp.concatenate(lefts, axis=1),
                jnp.concatenate(rights, axis=0),
                preferred_element_type=jnp.float32,
            )
            result.append(totals[s] + product)
        return tuple(result)

    block = right.shape[-1]
    zeros = tuple(jnp.zeros((block, block), jnp.float32) for _ in range(slots))
    return lax.fori_loop(0, (most + 1) // 2, step, zeros)


def stack(target, tiles):
    at = 0
    for tile in tiles:
        target[at : at + tile.shape[0]] = tile[...]
        at += tile.shape[0]


def early_square_kernel(sizes, early_count, *refs):
    slots, room = sizes[2], sizes[5]
    occ = refs[0]
    rights = refs[1 : 1 + early_count]
    lefts = (rights[0],) + refs[1 + early_count : -5]
    plan, partial, factors, left, right = refs[-5:]
    block = right.shape[-1]
    stack(right, rights)
    stack(left, lefts)
    left[left.shape[0] - 1] = jnp.zeros(left.shape[1:], left.dtype)
    factors[...] = jnp.zeros(factors.shape, factors.dtype)
    make_plan(sizes, occ, plan)
    sums = pair_sums(plan, room, left, right, slots)
    for s in range(slots):
        partial[s] = sums[s]

        def place(turn, carry, s=s):
            at = s * room + 1 + 2 * turn
            to = jnp.maximum(plan[at + 1] - right.shape[0], -1) + 1
            factors[to, s * block : (s + 1) * block, :] = left[plan[at]]
            return carry

        lax.fori_loop(0, plan[s * room], place, 0)


def late_square_kernel(sizes, factor, *refs):
    slots = sizes[2]
    partial, factors = refs[:2]
    rights = refs[2:-1]
    out = refs[-1]
    block = out.shape[-1]
    left = jnp.concatenate([factors[k] for k in range(1, factors.shape[0])], axis=1)
    right = jnp.concatenate([tile[u] for tile in rights for u in range(tile.shape[0])], axis=0)
    product = jnp.dot(left, right, preferred_element_type=jnp.float32)
    for s in range(slots):
        out[s] = (factor * (partial[s] + product[s * block : (s + 1) * block])).astype(out.dtype)


def early_cube_kernel(sizes, factor, right_count, *refs):
    slots, room = sizes[2], sizes[5]
    plan_in = refs[0]
    rights = refs[1 : 1 + right_count]
    lefts = refs[1 + right_count : 3 + right_count]
    square, partial, factors, left, right, plan, sem, square_sem = refs[3 + right_count :]
    square_copy = pltpu.make_async_copy(lefts[0], square, square_sem)
    square_copy.start()
    copy = pltpu.make_async_copy(plan_in, plan, sem)
    copy.start()
    early = len(lefts) * slots
    block = right.shape[-1]
    stack(right, rights)
    stack(left, lefts)
    left[early] = jnp.zeros(left.shape[1:], left.dtype)
    factors[...] = jnp.zeros(factors.shape, factors.dtype)
    copy.wait()
    sums = pair_sums(plan, room, left, right, slots)
    for s in range(slots):
        stored = plan[(s + 1) * room - 1].astype(jnp.float32)
        own = rights[0][s].astype(jnp.float32) * stored
        partial[s] = 1.5 * own - (0.5 * factor) * sums[s]

        def place(turn, carry, s=s):
            at = s * room + 1 + 2 * turn
            to = jnp.maximum(plan[at] - early, -1) + 1
            factors[to, :, s * block : (s + 1) * block] = right[plan[at + 1]]
            return carry

        lax.fori_loop(0, plan[s * room], place, 0)
    square_copy.wait()


def late_cube_kernel(sizes, factor, *refs):
    slots = sizes[2]
    partial, factors = refs[:2]
    lefts = refs[2:-3]
    updated, result, out_sem = refs[-3:]
    block = result.shape[-1]
    left = jnp.concatenate([tile[u] for tile in lefts for u in range(slots)], axis=1)
    right = factors[1:].reshape(left.shape[1], slots * block)
    product = jnp.dot(left, right, preferred_element_type=jnp.float32)
    copies = []
    for s in range(slots):
        result[s] = partial[s] - (0.5 * factor) * product[:, s * block : (s + 1) * block]
        copies.append(pltpu.make_async_copy(result.at[s], updated.at[s], out_sem.at[s]))
        copies[-1].start()
    for done in copies:
        done.wait()


def per_device(values, occupancy):
    row_count = lax.axis_size("row")
    col_count = lax.axis_size("col")
    slots = values.shape[2]
    block = values.shape[-1]
    tile_rows = RB
    tile_cols = RB * row_count // col_count
    factor = 5.0 / math.sqrt(tile_rows * block * row_count)
    room = 2 * (row_count * slots + 1) + 2
    sizes = (row_count, col_count, slots, tile_rows, tile_cols, room)
    tile = jax.ShapeDtypeStruct((slots, block, block), jnp.bfloat16)
    wide = jax.ShapeDtypeStruct((slots, block, block), jnp.float32)
    dma = pltpu.SemaphoreType.DMA
    plan_shape = ((slots * room,), jnp.int32)

    own = join(values.reshape(tile.shape))
    direct, forwarded, lefts = gather(own, row_count, col_count)
    early_rights = [own] + direct
    late_count = (row_count - len(early_rights)) * slots
    plan, partial, factors = pl.pallas_call(
        functools.partial(early_square_kernel, sizes, len(early_rights)),
        out_shape=(
            jax.ShapeDtypeStruct(*plan_shape),
            wide,
            jax.ShapeDtypeStruct((late_count + 1, slots * block, block), jnp.bfloat16),
        ),
        in_specs=[SMEM] + [VMEM] * (len(early_rights) + len(lefts)),
        out_specs=(SMEM, VMEM, VMEM),
        scratch_shapes=[
            pltpu.VMEM((col_count * slots + 1, block, block), jnp.bfloat16),
            pltpu.VMEM((len(early_rights) * slots, block, block), jnp.bfloat16),
        ],
        compiler_params=PARAMS,
        name="early_square",
    )(occupancy.transpose(1, 2, 0), *early_rights, *lefts)
    square = pl.pallas_call(
        functools.partial(late_square_kernel, sizes, factor),
        out_shape=tile,
        in_specs=[VMEM] * (2 + len(forwarded)),
        out_specs=VMEM,
        compiler_params=PARAMS,
        name="late_square",
    )(partial, factors, *forwarded)

    far = range(2, col_count, 2)
    others = {k: send(square, "col", k) for k in far}
    others[1] = send(square, "col", 1)
    for k in far:
        others[k + 1] = send(others[k], "col", 1)
    rights = early_rights + forwarded
    square_out, partial, factors = pl.pallas_call(
        functools.partial(early_cube_kernel, sizes, factor, len(rights)),
        out_shape=(tile, wide, jax.ShapeDtypeStruct(((col_count - 2) * slots + 1, block, slots * block), jnp.bfloat16)),
        in_specs=[ANY] + [VMEM] * (len(rights) + 2),
        out_specs=(ANY, VMEM, VMEM),
        scratch_shapes=[
            pltpu.VMEM((2 * slots + 1, block, block), jnp.bfloat16),
            pltpu.VMEM((row_count * slots, block, block), jnp.bfloat16),
            pltpu.SMEM(*plan_shape),
            dma,
            dma,
        ],
        compiler_params=PARAMS,
        name="early_cube",
    )(plan, *rights, square, others[1])
    updated = pl.pallas_call(
        functools.partial(late_cube_kernel, sizes, factor),
        out_shape=wide,
        in_specs=[VMEM] * col_count,
        out_specs=ANY,
        scratch_shapes=[pltpu.VMEM(wide.shape, jnp.float32), dma((slots,))],
        compiler_params=PARAMS,
        name="late_cube",
    )(partial, factors, *[others[k] for k in range(2, col_count)])
    shape_out = (1, 1) + tile.shape
    return (square_out.reshape(shape_out), updated.reshape(shape_out))


def solution(mesh):
    spec = P("row", "col", None, None, None)

    return jax.shard_map(
        per_device,
        mesh=mesh,
        in_specs=(spec, P()),
        out_specs=(spec, spec),
        check_vma=False,
    )
```

```python
import functools
import math

import jax
import jax.numpy as jnp
from jax import lax
from jax.experimental import pallas as pl
from jax.experimental.pallas import tpu as pltpu
from jax.sharding import PartitionSpec as P


RB = 2
PARAMS = pltpu.CompilerParams(vmem_limit_bytes=24 * 1024 * 1024)
VMEM = pl.BlockSpec(memory_space=pltpu.VMEM)
SMEM = pl.BlockSpec(memory_space=pltpu.SMEM)
ANY = pl.BlockSpec(memory_space=pl.ANY)


def send(array, axis, offset):
    size = lax.axis_size(axis)
    return lax.ppermute(array, axis, [(i, i ^ offset) for i in range(size)])


def join_kernel(*refs):
    at = 0
    for ref in refs[:-1]:
        refs[-1][at : at + ref.shape[0]] = ref[...]
        at += ref.shape[0]


def join(*arrays):
    shape = (sum(a.shape[0] for a in arrays),) + arrays[0].shape[1:]
    return pl.pallas_call(
        join_kernel,
        out_shape=jax.ShapeDtypeStruct(shape, arrays[0].dtype),
        in_specs=[VMEM] * len(arrays),
        out_specs=VMEM,
        compiler_params=PARAMS,
        name="join",
    )(*arrays)


def far_rows(row_count):
    return list(range(row_count - 4, 0, -4))


def column_order(row_count):
    far = far_rows(row_count)
    early = [0] + [g + 2 for g in far] + [2, 1] + [g + 1 for g in far]
    late = [3, far[0] + 3, far[0]]
    for g in far[1:]:
        late += [g + 3, g]
    return early, late


def gather(values, row_count, col_count):
    far = far_rows(row_count)
    rows = {k: send(values, "row", k) for k in [g + 2 for g in far] + [2]}
    near = send(values, "col", 1)
    for k in [1] + [g + 1 for g in far]:
        rows[k] = send(values, "row", k)
    direct = list(rows.values())
    own = join(values)
    pair = join(own, near)
    lefts = [near] + [send(pair, "col", k) for k in range(2, col_count, 2)]
    late = []
    for g in far:
        source = rows[g + 2]
        late.append(send(source if late else join(rows[2], source), "row", 1))
        late.append(send(source, "row", 2))
    return own, direct, late, lefts


def split(number, divisor):
    if divisor & (divisor - 1) == 0:
        return number >> (divisor.bit_length() - 1), number & (divisor - 1)
    return lax.div(number, divisor), lax.rem(number, divisor)


def plan_kernel(sizes, occ, plan):
    row_count, _, slots, tile_rows, tile_cols, room = sizes
    row, col = lax.axis_index("row"), lax.axis_index("col")
    positions = tile_rows * tile_cols
    mine = [occ[col, s, row] for s in range(slots)]
    lines = [split(q, tile_cols) for q in mine]
    lines = [(line * tile_cols, jnp.where(q < positions, c, -1)) for q, (line, c) in zip(mine, lines)]
    ends = [jnp.int32(s * room + 1) for s in range(slots)]
    early, late = column_order(row_count)
    for at, offset in enumerate(early + late):
        tile = row ^ offset
        for u in range(slots):
            q = occ[col, u, tile]
            line, column = split(q, tile_cols)
            panel, depth = split(tile * tile_rows + jnp.minimum(line, tile_rows - 1), tile_cols)
            column = jnp.where(q < positions, column, -2)
            base = (panel ^ col) * slots
            held = [occ[panel, v, row] for v in range(slots)]
            for s in range(slots):
                wanted = jnp.where(lines[s][1] == column, lines[s][0] + depth, -1)
                place = base
                hit = held[0] == wanted
                for v in range(1, slots):
                    also = held[v] == wanted
                    place = jnp.where(also, base + v, place)
                    hit = hit | also
                plan[ends[s]] = place
                plan[ends[s] + 1] = jnp.int32(at * slots + u)
                ends[s] = ends[s] + jnp.where(hit, 2, 0)
    for s in range(slots):
        plan[s * room] = (ends[s] - (s * room + 1)) >> 1
        plan[(s + 1) * room - 1] = (mine[s] < positions).astype(jnp.int32)
        plan[ends[s]] = jnp.int32(0)
        plan[ends[s] + 1] = jnp.int32(0)


def pair_sums(plan, room, left, right, slots):
    counts = [plan[s * room] for s in range(slots)]
    most = functools.reduce(jnp.maximum, counts)
    zero_block = left.shape[0] - 1
    last = right.shape[0] - 1

    def step(turn, totals):
        result = []
        for s in range(slots):
            lefts, rights = [], []
            for half in range(2):
                at = 2 * turn + half
                live = at < counts[s]
                at = s * room + 1 + 2 * jnp.minimum(at, counts[s])
                place, other = plan[at], plan[at + 1]
                live = live & (place < zero_block) & (other <= last)
                lefts.append(left[jnp.where(live, place, zero_block)])
                rights.append(right[jnp.minimum(other, last)])
            product = jnp.dot(
                jnp.concatenate(lefts, axis=1),
                jnp.concatenate(rights, axis=0),
                preferred_element_type=jnp.float32,
            )
            result.append(totals[s] + product)
        return tuple(result)

    block = right.shape[-1]
    zeros = tuple(jnp.zeros((block, block), jnp.float32) for _ in range(slots))
    return lax.fori_loop(0, (most + 1) // 2, step, zeros)


def stack(target, tiles):
    at = 0
    for tile in tiles:
        target[at : at + tile.shape[0]] = tile[...]
        at += tile.shape[0]


def early_square_kernel(sizes, early_count, *refs):
    slots, room = sizes[2], sizes[5]
    rights = refs[1 : 1 + early_count]
    lefts = (rights[0],) + refs[1 + early_count : -6]
    partial, factors, left, right, plan, sem = refs[-6:]
    block = right.shape[-1]
    copy = pltpu.make_async_copy(refs[0], plan, sem)
    copy.start()
    stack(right, rights)
    stack(left, lefts)
    left[left.shape[0] - 1] = jnp.zeros(left.shape[1:], left.dtype)
    factors[...] = jnp.zeros(factors.shape, factors.dtype)
    copy.wait()
    sums = pair_sums(plan, room, left, right, slots)
    for s in range(slots):
        partial[s] = sums[s]

        def place(turn, carry, s=s):
            at = s * room + 1 + 2 * turn
            to = jnp.maximum(plan[at + 1] - right.shape[0], -1) + 1
            factors[to, s * block : (s + 1) * block, :] = left[plan[at]]
            return carry

        lax.fori_loop(0, plan[s * room], place, 0)


def late_square_kernel(sizes, factor, *refs):
    slots = sizes[2]
    partial, factors = refs[:2]
    rights = refs[2:-1]
    out = refs[-1]
    block = out.shape[-1]
    left = jnp.concatenate([factors[k] for k in range(1, factors.shape[0])], axis=1)
    right = jnp.concatenate([tile[u] for tile in rights for u in range(tile.shape[0])], axis=0)
    product = jnp.dot(left, right, preferred_element_type=jnp.float32)
    for s in range(slots):
        out[s] = (factor * (partial[s] + product[s * block : (s + 1) * block])).astype(out.dtype)


def early_cube_kernel(sizes, factor, right_count, *refs):
    slots, room = sizes[2], sizes[5]
    plan_in = refs[0]
    rights = refs[1 : 1 + right_count]
    lefts = refs[1 + right_count : 3 + right_count]
    square, partial, factors, left, right, plan, sem, square_sem = refs[3 + right_count :]
    square_copy = pltpu.make_async_copy(lefts[0], square, square_sem)
    square_copy.start()
    copy = pltpu.make_async_copy(plan_in, plan, sem)
    copy.start()
    early = len(lefts) * slots
    block = right.shape[-1]
    stack(right, rights)
    stack(left, lefts)
    left[early] = jnp.zeros(left.shape[1:], left.dtype)
    factors[...] = jnp.zeros(factors.shape, factors.dtype)
    copy.wait()
    sums = pair_sums(plan, room, left, right, slots)
    for s in range(slots):
        stored = plan[(s + 1) * room - 1].astype(jnp.float32)
        own = rights[0][s].astype(jnp.float32) * stored
        partial[s] = 1.5 * own - (0.5 * factor) * sums[s]

        def place(turn, carry, s=s):
            at = s * room + 1 + 2 * turn
            to = jnp.maximum(plan[at] - early, -1) + 1
            factors[to, :, s * block : (s + 1) * block] = right[plan[at + 1]]
            return carry

        lax.fori_loop(0, plan[s * room], place, 0)
    square_copy.wait()


def late_cube_kernel(sizes, factor, *refs):
    slots = sizes[2]
    partial, factors = refs[:2]
    lefts = refs[2:-3]
    updated, result, out_sem = refs[-3:]
    block = result.shape[-1]
    left = jnp.concatenate([tile[u] for tile in lefts for u in range(slots)], axis=1)
    right = factors[1:].reshape(left.shape[1], slots * block)
    product = jnp.dot(left, right, preferred_element_type=jnp.float32)
    copies = []
    for s in range(slots):
        result[s] = partial[s] - (0.5 * factor) * product[:, s * block : (s + 1) * block]
        copies.append(pltpu.make_async_copy(result.at[s], updated.at[s], out_sem.at[s]))
        copies[-1].start()
    for done in copies:
        done.wait()


def per_device(values, occupancy):
    row_count = lax.axis_size("row")
    col_count = lax.axis_size("col")
    slots = values.shape[2]
    block = values.shape[-1]
    tile_rows = RB
    tile_cols = RB * row_count // col_count
    factor = 5.0 / math.sqrt(tile_rows * block * row_count)
    room = 2 * (row_count * slots + 1) + 2
    sizes = (row_count, col_count, slots, tile_rows, tile_cols, room)
    tile = jax.ShapeDtypeStruct((slots, block, block), jnp.bfloat16)
    wide = jax.ShapeDtypeStruct((slots, block, block), jnp.float32)
    dma = pltpu.SemaphoreType.DMA
    plan_shape = ((slots * room,), jnp.int32)

    own, direct, forwarded, lefts = gather(values.reshape(tile.shape), row_count, col_count)
    early_rights = [own] + direct
    late_count = (row_count - len(early_rights)) * slots
    plan = pl.pallas_call(
        functools.partial(plan_kernel, sizes),
        out_shape=jax.ShapeDtypeStruct(*plan_shape),
        in_specs=[SMEM],
        out_specs=SMEM,
        compiler_params=PARAMS,
        name="plan",
    )(occupancy.transpose(1, 2, 0))
    partial, factors = pl.pallas_call(
        functools.partial(early_square_kernel, sizes, len(early_rights)),
        out_shape=(wide, jax.ShapeDtypeStruct((late_count + 1, slots * block, block), jnp.bfloat16)),
        in_specs=[ANY] + [VMEM] * (len(early_rights) + len(lefts)),
        out_specs=(VMEM, VMEM),
        scratch_shapes=[
            pltpu.VMEM((col_count * slots + 1, block, block), jnp.bfloat16),
            pltpu.VMEM((len(early_rights) * slots, block, block), jnp.bfloat16),
            pltpu.SMEM(*plan_shape),
            dma,
        ],
        compiler_params=PARAMS,
        name="early_square",
    )(plan, *early_rights, *lefts)
    square = pl.pallas_call(
        functools.partial(late_square_kernel, sizes, factor),
        out_shape=tile,
        in_specs=[VMEM] * (2 + len(forwarded)),
        out_specs=VMEM,
        compiler_params=PARAMS,
        name="late_square",
    )(partial, factors, *forwarded)

    far = range(2, col_count, 2)
    others = {k: send(square, "col", k) for k in far}
    others[1] = send(square, "col", 1)
    for k in far:
        others[k + 1] = send(others[k], "col", 1)
    rights = early_rights + forwarded
    square_out, partial, factors = pl.pallas_call(
        functools.partial(early_cube_kernel, sizes, factor, len(rights)),
        out_shape=(tile, wide, jax.ShapeDtypeStruct(((col_count - 2) * slots + 1, block, slots * block), jnp.bfloat16)),
        in_specs=[ANY] + [VMEM] * (len(rights) + 2),
        out_specs=(ANY, VMEM, VMEM),
        scratch_shapes=[
            pltpu.VMEM((2 * slots + 1, block, block), jnp.bfloat16),
            pltpu.VMEM((row_count * slots, block, block), jnp.bfloat16),
            pltpu.SMEM(*plan_shape),
            dma,
            dma,
        ],
        compiler_params=PARAMS,
        name="early_cube",
    )(plan, *rights, square, others[1])
    updated = pl.pallas_call(
        functools.partial(late_cube_kernel, sizes, factor),
        out_shape=wide,
        in_specs=[VMEM] * col_count,
        out_specs=ANY,
        scratch_shapes=[pltpu.VMEM(wide.shape, jnp.float32), dma((slots,))],
        compiler_params=PARAMS,
        name="late_cube",
    )(partial, factors, *[others[k] for k in range(2, col_count)])
    shape_out = (1, 1) + tile.shape
    return (square_out.reshape(shape_out), updated.reshape(shape_out))


def solution(mesh):
    spec = P("row", "col", None, None, None)

    return jax.shard_map(
        per_device,
        mesh=mesh,
        in_specs=(spec, P()),
        out_specs=(spec, spec),
        check_vma=False,
    )
```

```python
import functools
import math

import jax
import jax.numpy as jnp
from jax import lax
from jax.experimental import pallas as pl
from jax.experimental.pallas import tpu as pltpu
from jax.sharding import PartitionSpec as P


RB = 2
PARAMS = pltpu.CompilerParams(vmem_limit_bytes=24 * 1024 * 1024)
VMEM = pl.BlockSpec(memory_space=pltpu.VMEM)
SMEM = pl.BlockSpec(memory_space=pltpu.SMEM)
ANY = pl.BlockSpec(memory_space=pl.ANY)


def send(array, axis, offset):
    size = lax.axis_size(axis)
    return lax.ppermute(array, axis, [(i, i ^ offset) for i in range(size)])


def join_kernel(*refs):
    at = 0
    for ref in refs[:-1]:
        refs[-1][at : at + ref.shape[0]] = ref[...]
        at += ref.shape[0]


def join(*arrays):
    shape = (sum(a.shape[0] for a in arrays),) + arrays[0].shape[1:]
    return pl.pallas_call(
        join_kernel,
        out_shape=jax.ShapeDtypeStruct(shape, arrays[0].dtype),
        in_specs=[VMEM] * len(arrays),
        out_specs=VMEM,
        compiler_params=PARAMS,
        name="join",
    )(*arrays)


def far_rows(row_count):
    return list(range(row_count - 4, 0, -4))


def column_order(row_count):
    far = far_rows(row_count)
    early = [0] + [g + 2 for g in far] + [1, 2]
    late = [3, far[0], far[0] + 3]
    for g in far[1:]:
        late += [g, g + 3]
    return early, late + [g + 1 for g in far]


def gather(values, row_count, col_count):
    far = far_rows(row_count)
    rows = {k: send(values, "row", k) for k in [g + 2 for g in far] + [1]}
    near = send(values, "col", 1)
    rows[2] = send(values, "row", 2)
    direct = list(rows.values())
    slow = [send(values, "row", g + 1) for g in far]
    own = join(values)
    lefts = [near]
    for k in range(2, col_count, 2):
        lefts.append(send(values, "col", k))
        lefts.append(send(lefts[-1], "col", 1))
    late = []
    for g in far:
        source = rows[g + 2]
        late.append(send(source if late else join(rows[1], source), "row", 2))
        late.append(send(source, "row", 1))
    return own, direct, late + slow, lefts


def split(number, divisor):
    if divisor & (divisor - 1) == 0:
        return number >> (divisor.bit_length() - 1), number & (divisor - 1)
    return lax.div(number, divisor), lax.rem(number, divisor)


def plan_kernel(sizes, occ, plan):
    row_count, _, slots, tile_rows, tile_cols, room = sizes
    row, col = lax.axis_index("row"), lax.axis_index("col")
    positions = tile_rows * tile_cols
    mine = [occ[col, s, row] for s in range(slots)]
    lines = [split(q, tile_cols) for q in mine]
    lines = [(line * tile_cols, jnp.where(q < positions, c, -1)) for q, (line, c) in zip(mine, lines)]
    ends = [jnp.int32(s * room + 1) for s in range(slots)]
    early, late = column_order(row_count)
    for at, offset in enumerate(early + late):
        tile = row ^ offset
        for u in range(slots):
            q = occ[col, u, tile]
            line, column = split(q, tile_cols)
            panel, depth = split(tile * tile_rows + jnp.minimum(line, tile_rows - 1), tile_cols)
            column = jnp.where(q < positions, column, -2)
            base = (panel ^ col) * slots
            held = [occ[panel, v, row] for v in range(slots)]
            for s in range(slots):
                wanted = jnp.where(lines[s][1] == column, lines[s][0] + depth, -1)
                place = base
                hit = held[0] == wanted
                for v in range(1, slots):
                    also = held[v] == wanted
                    place = jnp.where(also, base + v, place)
                    hit = hit | also
                plan[ends[s]] = place
                plan[ends[s] + 1] = jnp.int32(at * slots + u)
                ends[s] = ends[s] + jnp.where(hit, 2, 0)
    for s in range(slots):
        plan[s * room] = (ends[s] - (s * room + 1)) >> 1
        plan[(s + 1) * room - 1] = (mine[s] < positions).astype(jnp.int32)
        plan[ends[s]] = jnp.int32(0)
        plan[ends[s] + 1] = jnp.int32(0)


def pair_sums(plan, room, left, right, slots):
    counts = [plan[s * room] for s in range(slots)]
    most = functools.reduce(jnp.maximum, counts)
    zero_block = left.shape[0] - 1
    last = right.shape[0] - 1

    def step(turn, totals):
        result = []
        for s in range(slots):
            lefts, rights = [], []
            for half in range(2):
                at = 2 * turn + half
                live = at < counts[s]
                at = s * room + 1 + 2 * jnp.minimum(at, counts[s])
                place, other = plan[at], plan[at + 1]
                live = live & (place < zero_block) & (other <= last)
                lefts.append(left[jnp.where(live, place, zero_block)])
                rights.append(right[jnp.minimum(other, last)])
            product = jnp.dot(
                jnp.concatenate(lefts, axis=1),
                jnp.concatenate(rights, axis=0),
                preferred_element_type=jnp.float32,
            )
            result.append(totals[s] + product)
        return tuple(result)

    block = right.shape[-1]
    zeros = tuple(jnp.zeros((block, block), jnp.float32) for _ in range(slots))
    return lax.fori_loop(0, (most + 1) // 2, step, zeros)


def stack(target, tiles):
    at = 0
    for tile in tiles:
        target[at : at + tile.shape[0]] = tile[...]
        at += tile.shape[0]


def early_square_kernel(sizes, early_count, *refs):
    slots, room = sizes[2], sizes[5]
    rights = refs[1 : 1 + early_count]
    lefts = (rights[0],) + refs[1 + early_count : -6]
    partial, factors, left, right, plan, sem = refs[-6:]
    block = right.shape[-1]
    copy = pltpu.make_async_copy(refs[0], plan, sem)
    copy.start()
    stack(right, rights)
    stack(left, lefts)
    left[left.shape[0] - 1] = jnp.zeros(left.shape[1:], left.dtype)
    factors[...] = jnp.zeros(factors.shape, factors.dtype)
    copy.wait()
    sums = pair_sums(plan, room, left, right, slots)
    for s in range(slots):
        partial[s] = sums[s]

        def place(turn, carry, s=s):
            at = s * room + 1 + 2 * turn
            to = jnp.maximum(plan[at + 1] - right.shape[0], -1) + 1
            factors[to, s * block : (s + 1) * block, :] = left[plan[at]]
            return carry

        lax.fori_loop(0, plan[s * room], place, 0)


def late_square_kernel(sizes, factor, *refs):
    slots = sizes[2]
    partial, factors = refs[:2]
    rights = refs[2:-1]
    out = refs[-1]
    block = out.shape[-1]
    left = jnp.concatenate([factors[k] for k in range(1, factors.shape[0])], axis=1)
    right = jnp.concatenate([tile[u] for tile in rights for u in range(tile.shape[0])], axis=0)
    product = jnp.dot(left, right, preferred_element_type=jnp.float32)
    for s in range(slots):
        out[s] = (factor * (partial[s] + product[s * block : (s + 1) * block])).astype(out.dtype)


def early_cube_kernel(sizes, factor, right_count, *refs):
    slots, room = sizes[2], sizes[5]
    plan_in = refs[0]
    rights = refs[1 : 1 + right_count]
    lefts = refs[1 + right_count : 3 + right_count]
    square, partial, factors, left, right, plan, sem, square_sem = refs[3 + right_count :]
    square_copy = pltpu.make_async_copy(lefts[0], square, square_sem)
    square_copy.start()
    copy = pltpu.make_async_copy(plan_in, plan, sem)
    copy.start()
    early = len(lefts) * slots
    block = right.shape[-1]
    stack(right, rights)
    stack(left, lefts)
    left[early] = jnp.zeros(left.shape[1:], left.dtype)
    factors[...] = jnp.zeros(factors.shape, factors.dtype)
    copy.wait()
    sums = pair_sums(plan, room, left, right, slots)
    for s in range(slots):
        stored = plan[(s + 1) * room - 1].astype(jnp.float32)
        own = rights[0][s].astype(jnp.float32) * stored
        partial[s] = 1.5 * own - (0.5 * factor) * sums[s]

        def place(turn, carry, s=s):
            at = s * room + 1 + 2 * turn
            to = jnp.maximum(plan[at] - early, -1) + 1
            factors[to, :, s * block : (s + 1) * block] = right[plan[at + 1]]
            return carry

        lax.fori_loop(0, plan[s * room], place, 0)
    square_copy.wait()


def late_cube_kernel(sizes, factor, *refs):
    slots = sizes[2]
    partial, factors = refs[:2]
    lefts = refs[2:-3]
    updated, result, out_sem = refs[-3:]
    block = result.shape[-1]
    left = jnp.concatenate([tile[u] for tile in lefts for u in range(slots)], axis=1)
    right = factors[1:].reshape(left.shape[1], slots * block)
    product = jnp.dot(left, right, preferred_element_type=jnp.float32)
    copies = []
    for s in range(slots):
        result[s] = partial[s] - (0.5 * factor) * product[:, s * block : (s + 1) * block]
        copies.append(pltpu.make_async_copy(result.at[s], updated.at[s], out_sem.at[s]))
        copies[-1].start()
    for done in copies:
        done.wait()


def per_device(values, occupancy):
    row_count = lax.axis_size("row")
    col_count = lax.axis_size("col")
    slots = values.shape[2]
    block = values.shape[-1]
    tile_rows = RB
    tile_cols = RB * row_count // col_count
    factor = 5.0 / math.sqrt(tile_rows * block * row_count)
    room = 2 * (row_count * slots + 1) + 2
    sizes = (row_count, col_count, slots, tile_rows, tile_cols, room)
    tile = jax.ShapeDtypeStruct((slots, block, block), jnp.bfloat16)
    wide = jax.ShapeDtypeStruct((slots, block, block), jnp.float32)
    dma = pltpu.SemaphoreType.DMA
    plan_shape = ((slots * room,), jnp.int32)

    own, direct, forwarded, lefts = gather(values.reshape(tile.shape), row_count, col_count)
    early_rights = [own] + direct
    late_count = (row_count - len(early_rights)) * slots
    plan = pl.pallas_call(
        functools.partial(plan_kernel, sizes),
        out_shape=jax.ShapeDtypeStruct(*plan_shape),
        in_specs=[SMEM],
        out_specs=SMEM,
        compiler_params=PARAMS,
        name="plan",
    )(occupancy.transpose(1, 2, 0))
    partial, factors = pl.pallas_call(
        functools.partial(early_square_kernel, sizes, len(early_rights)),
        out_shape=(wide, jax.ShapeDtypeStruct((late_count + 1, slots * block, block), jnp.bfloat16)),
        in_specs=[ANY] + [VMEM] * (len(early_rights) + len(lefts)),
        out_specs=(VMEM, VMEM),
        scratch_shapes=[
            pltpu.VMEM((col_count * slots + 1, block, block), jnp.bfloat16),
            pltpu.VMEM((len(early_rights) * slots, block, block), jnp.bfloat16),
            pltpu.SMEM(*plan_shape),
            dma,
        ],
        compiler_params=PARAMS,
        name="early_square",
    )(plan, *early_rights, *lefts)
    square = pl.pallas_call(
        functools.partial(late_square_kernel, sizes, factor),
        out_shape=tile,
        in_specs=[VMEM] * (2 + len(forwarded)),
        out_specs=VMEM,
        compiler_params=PARAMS,
        name="late_square",
    )(partial, factors, *forwarded)

    far = range(2, col_count, 2)
    others = {k: send(square, "col", k) for k in far}
    others[1] = send(square, "col", 1)
    for k in far:
        others[k + 1] = send(others[k], "col", 1)
    rights = early_rights + forwarded
    square_out, partial, factors = pl.pallas_call(
        functools.partial(early_cube_kernel, sizes, factor, len(rights)),
        out_shape=(tile, wide, jax.ShapeDtypeStruct(((col_count - 2) * slots + 1, block, slots * block), jnp.bfloat16)),
        in_specs=[ANY] + [VMEM] * (len(rights) + 2),
        out_specs=(ANY, VMEM, VMEM),
        scratch_shapes=[
            pltpu.VMEM((2 * slots + 1, block, block), jnp.bfloat16),
            pltpu.VMEM((row_count * slots, block, block), jnp.bfloat16),
            pltpu.SMEM(*plan_shape),
            dma,
            dma,
        ],
        compiler_params=PARAMS,
        name="early_cube",
    )(plan, *rights, square, others[1])
    updated = pl.pallas_call(
        functools.partial(late_cube_kernel, sizes, factor),
        out_shape=wide,
        in_specs=[VMEM] * col_count,
        out_specs=ANY,
        scratch_shapes=[pltpu.VMEM(wide.shape, jnp.float32), dma((slots,))],
        compiler_params=PARAMS,
        name="late_cube",
    )(partial, factors, *[others[k] for k in range(2, col_count)])
    shape_out = (1, 1) + tile.shape
    return (square_out.reshape(shape_out), updated.reshape(shape_out))


def solution(mesh):
    spec = P("row", "col", None, None, None)

    return jax.shard_map(
        per_device,
        mesh=mesh,
        in_specs=(spec, P()),
        out_specs=(spec, spec),
        check_vma=False,
    )
```

```python
import functools
import math

import jax
import jax.numpy as jnp
from jax import lax
from jax.experimental import pallas as pl
from jax.experimental.pallas import tpu as pltpu
from jax.sharding import PartitionSpec as P


RB = 2
PARAMS = pltpu.CompilerParams(vmem_limit_bytes=24 * 1024 * 1024)
VMEM = pl.BlockSpec(memory_space=pltpu.VMEM)
SMEM = pl.BlockSpec(memory_space=pltpu.SMEM)
ANY = pl.BlockSpec(memory_space=pl.ANY)


def send(array, axis, offset):
    size = lax.axis_size(axis)
    return lax.ppermute(array, axis, [(i, i ^ offset) for i in range(size)])


def join_kernel(*refs):
    at = 0
    for ref in refs[:-1]:
        refs[-1][at : at + ref.shape[0]] = ref[...]
        at += ref.shape[0]


def join(*arrays):
    shape = (sum(a.shape[0] for a in arrays),) + arrays[0].shape[1:]
    return pl.pallas_call(
        join_kernel,
        out_shape=jax.ShapeDtypeStruct(shape, arrays[0].dtype),
        in_specs=[VMEM] * len(arrays),
        out_specs=VMEM,
        compiler_params=PARAMS,
        name="join",
    )(*arrays)


def far_rows(row_count):
    return list(range(row_count - 4, 0, -4))


def column_order(row_count):
    far = far_rows(row_count)
    early = [0] + [g + 2 for g in far] + [1, 2]
    late = [3, far[0], far[0] + 3]
    for g in far[1:]:
        late += [g, g + 3]
    return early, late + [g + 1 for g in far]


def gather(values, row_count, col_count):
    far = far_rows(row_count)
    rows = {k: send(values, "row", k) for k in [g + 2 for g in far] + [1]}
    near = send(values, "col", 1)
    rows[2] = send(values, "row", 2)
    direct = list(rows.values())
    slow = [send(values, "row", g + 1) for g in far]
    own = join(values)
    lefts = [near]
    for k in range(2, col_count, 2):
        cross = send(values, "col", k + 1)
        lefts += [send(cross, "col", 1), cross]
    late = []
    for g in far:
        source = rows[g + 2]
        late.append(send(source if late else join(rows[1], source), "row", 2))
        late.append(send(source, "row", 1))
    return own, direct, late + slow, lefts


def split(number, divisor):
    if divisor & (divisor - 1) == 0:
        return number >> (divisor.bit_length() - 1), number & (divisor - 1)
    return lax.div(number, divisor), lax.rem(number, divisor)


def plan_kernel(sizes, occ, plan):
    row_count, _, slots, tile_rows, tile_cols, room = sizes
    row, col = lax.axis_index("row"), lax.axis_index("col")
    positions = tile_rows * tile_cols
    mine = [occ[col, s, row] for s in range(slots)]
    lines = [split(q, tile_cols) for q in mine]
    lines = [(line * tile_cols, jnp.where(q < positions, c, -1)) for q, (line, c) in zip(mine, lines)]
    ends = [jnp.int32(s * room + 1) for s in range(slots)]
    early, late = column_order(row_count)
    for at, offset in enumerate(early + late):
        tile = row ^ offset
        for u in range(slots):
            q = occ[col, u, tile]
            line, column = split(q, tile_cols)
            panel, depth = split(tile * tile_rows + jnp.minimum(line, tile_rows - 1), tile_cols)
            column = jnp.where(q < positions, column, -2)
            base = (panel ^ col) * slots
            held = [occ[panel, v, row] for v in range(slots)]
            for s in range(slots):
                wanted = jnp.where(lines[s][1] == column, lines[s][0] + depth, -1)
                place = base
                hit = held[0] == wanted
                for v in range(1, slots):
                    also = held[v] == wanted
                    place = jnp.where(also, base + v, place)
                    hit = hit | also
                plan[ends[s]] = place
                plan[ends[s] + 1] = jnp.int32(at * slots + u)
                ends[s] = ends[s] + jnp.where(hit, 2, 0)
    for s in range(slots):
        plan[s * room] = (ends[s] - (s * room + 1)) >> 1
        plan[(s + 1) * room - 1] = (mine[s] < positions).astype(jnp.int32)
        plan[ends[s]] = jnp.int32(0)
        plan[ends[s] + 1] = jnp.int32(0)


def pair_sums(plan, room, left, right, slots):
    counts = [plan[s * room] for s in range(slots)]
    most = functools.reduce(jnp.maximum, counts)
    zero_block = left.shape[0] - 1
    last = right.shape[0] - 1

    def step(turn, totals):
        result = []
        for s in range(slots):
            lefts, rights = [], []
            for half in range(2):
                at = 2 * turn + half
                live = at < counts[s]
                at = s * room + 1 + 2 * jnp.minimum(at, counts[s])
                place, other = plan[at], plan[at + 1]
                live = live & (place < zero_block) & (other <= last)
                lefts.append(left[jnp.where(live, place, zero_block)])
                rights.append(right[jnp.minimum(other, last)])
            product = jnp.dot(
                jnp.concatenate(lefts, axis=1),
                jnp.concatenate(rights, axis=0),
                preferred_element_type=jnp.float32,
            )
            result.append(totals[s] + product)
        return tuple(result)

    block = right.shape[-1]
    zeros = tuple(jnp.zeros((block, block), jnp.float32) for _ in range(slots))
    return lax.fori_loop(0, (most + 1) // 2, step, zeros)


def stack(target, tiles):
    at = 0
    for tile in tiles:
        target[at : at + tile.shape[0]] = tile[...]
        at += tile.shape[0]


def early_square_kernel(sizes, early_count, *refs):
    slots, room = sizes[2], sizes[5]
    rights = refs[1 : 1 + early_count]
    lefts = (rights[0],) + refs[1 + early_count : -6]
    partial, factors, left, right, plan, sem = refs[-6:]
    block = right.shape[-1]
    copy = pltpu.make_async_copy(refs[0], plan, sem)
    copy.start()
    stack(right, rights)
    stack(left, lefts)
    left[left.shape[0] - 1] = jnp.zeros(left.shape[1:], left.dtype)
    factors[...] = jnp.zeros(factors.shape, factors.dtype)
    copy.wait()
    sums = pair_sums(plan, room, left, right, slots)
    for s in range(slots):
        partial[s] = sums[s]

        def place(turn, carry, s=s):
            at = s * room + 1 + 2 * turn
            to = jnp.maximum(plan[at + 1] - right.shape[0], -1) + 1
            factors[to, s * block : (s + 1) * block, :] = left[plan[at]]
            return carry

        lax.fori_loop(0, plan[s * room], place, 0)


def late_square_kernel(sizes, factor, *refs):
    slots = sizes[2]
    partial, factors = refs[:2]
    rights = refs[2:-1]
    out = refs[-1]
    block = out.shape[-1]
    left = jnp.concatenate([factors[k] for k in range(1, factors.shape[0])], axis=1)
    right = jnp.concatenate([tile[u] for tile in rights for u in range(tile.shape[0])], axis=0)
    product = jnp.dot(left, right, preferred_element_type=jnp.float32)
    for s in range(slots):
        out[s] = (factor * (partial[s] + product[s * block : (s + 1) * block])).astype(out.dtype)


def early_cube_kernel(sizes, factor, right_count, *refs):
    slots, room = sizes[2], sizes[5]
    plan_in = refs[0]
    rights = refs[1 : 1 + right_count]
    lefts = refs[1 + right_count : 3 + right_count]
    square, partial, factors, left, right, plan, sem, square_sem = refs[3 + right_count :]
    square_copy = pltpu.make_async_copy(lefts[0], square, square_sem)
    square_copy.start()
    copy = pltpu.make_async_copy(plan_in, plan, sem)
    copy.start()
    early = len(lefts) * slots
    block = right.shape[-1]
    stack(right, rights)
    stack(left, lefts)
    left[early] = jnp.zeros(left.shape[1:], left.dtype)
    factors[...] = jnp.zeros(factors.shape, factors.dtype)
    copy.wait()
    sums = pair_sums(plan, room, left, right, slots)
    for s in range(slots):
        stored = plan[(s + 1) * room - 1].astype(jnp.float32)
        own = rights[0][s].astype(jnp.float32) * stored
        partial[s] = 1.5 * own - (0.5 * factor) * sums[s]

        def place(turn, carry, s=s):
            at = s * room + 1 + 2 * turn
            to = jnp.maximum(plan[at] - early, -1) + 1
            factors[to, :, s * block : (s + 1) * block] = right[plan[at + 1]]
            return carry

        lax.fori_loop(0, plan[s * room], place, 0)
    square_copy.wait()


def late_cube_kernel(sizes, factor, *refs):
    slots = sizes[2]
    partial, factors = refs[:2]
    lefts = refs[2:-3]
    updated, result, out_sem = refs[-3:]
    block = result.shape[-1]
    left = jnp.concatenate([tile[u] for tile in lefts for u in range(slots)], axis=1)
    right = factors[1:].reshape(left.shape[1], slots * block)
    product = jnp.dot(left, right, preferred_element_type=jnp.float32)
    copies = []
    for s in range(slots):
        result[s] = partial[s] - (0.5 * factor) * product[:, s * block : (s + 1) * block]
        copies.append(pltpu.make_async_copy(result.at[s], updated.at[s], out_sem.at[s]))
        copies[-1].start()
    for done in copies:
        done.wait()


def per_device(values, occupancy):
    row_count = lax.axis_size("row")
    col_count = lax.axis_size("col")
    slots = values.shape[2]
    block = values.shape[-1]
    tile_rows = RB
    tile_cols = RB * row_count // col_count
    factor = 5.0 / math.sqrt(tile_rows * block * row_count)
    room = 2 * (row_count * slots + 1) + 2
    sizes = (row_count, col_count, slots, tile_rows, tile_cols, room)
    tile = jax.ShapeDtypeStruct((slots, block, block), jnp.bfloat16)
    wide = jax.ShapeDtypeStruct((slots, block, block), jnp.float32)
    dma = pltpu.SemaphoreType.DMA
    plan_shape = ((slots * room,), jnp.int32)

    own, direct, forwarded, lefts = gather(values.reshape(tile.shape), row_count, col_count)
    early_rights = [own] + direct
    late_count = (row_count - len(early_rights)) * slots
    plan = pl.pallas_call(
        functools.partial(plan_kernel, sizes),
        out_shape=jax.ShapeDtypeStruct(*plan_shape),
        in_specs=[SMEM],
        out_specs=SMEM,
        compiler_params=PARAMS,
        name="plan",
    )(occupancy.transpose(1, 2, 0))
    partial, factors = pl.pallas_call(
        functools.partial(early_square_kernel, sizes, len(early_rights)),
        out_shape=(wide, jax.ShapeDtypeStruct((late_count + 1, slots * block, block), jnp.bfloat16)),
        in_specs=[ANY] + [VMEM] * (len(early_rights) + len(lefts)),
        out_specs=(VMEM, VMEM),
        scratch_shapes=[
            pltpu.VMEM((col_count * slots + 1, block, block), jnp.bfloat16),
            pltpu.VMEM((len(early_rights) * slots, block, block), jnp.bfloat16),
            pltpu.SMEM(*plan_shape),
            dma,
        ],
        compiler_params=PARAMS,
        name="early_square",
    )(plan, *early_rights, *lefts)
    square = pl.pallas_call(
        functools.partial(late_square_kernel, sizes, factor),
        out_shape=tile,
        in_specs=[VMEM] * (2 + len(forwarded)),
        out_specs=VMEM,
        compiler_params=PARAMS,
        name="late_square",
    )(partial, factors, *forwarded)

    far = range(2, col_count, 2)
    others = {k + 1: send(square, "col", k + 1) for k in far}
    others[1] = send(square, "col", 1)
    for k in far:
        others[k] = send(others[k + 1], "col", 1)
    rights = early_rights + forwarded
    square_out, partial, factors = pl.pallas_call(
        functools.partial(early_cube_kernel, sizes, factor, len(rights)),
        out_shape=(tile, wide, jax.ShapeDtypeStruct(((col_count - 2) * slots + 1, block, slots * block), jnp.bfloat16)),
        in_specs=[ANY] + [VMEM] * (len(rights) + 2),
        out_specs=(ANY, VMEM, VMEM),
        scratch_shapes=[
            pltpu.VMEM((2 * slots + 1, block, block), jnp.bfloat16),
            pltpu.VMEM((row_count * slots, block, block), jnp.bfloat16),
            pltpu.SMEM(*plan_shape),
            dma,
            dma,
        ],
        compiler_params=PARAMS,
        name="early_cube",
    )(plan, *rights, square, others[1])
    updated = pl.pallas_call(
        functools.partial(late_cube_kernel, sizes, factor),
        out_shape=wide,
        in_specs=[VMEM] * col_count,
        out_specs=ANY,
        scratch_shapes=[pltpu.VMEM(wide.shape, jnp.float32), dma((slots,))],
        compiler_params=PARAMS,
        name="late_cube",
    )(partial, factors, *[others[k] for k in range(2, col_count)])
    shape_out = (1, 1) + tile.shape
    return (square_out.reshape(shape_out), updated.reshape(shape_out))


def solution(mesh):
    spec = P("row", "col", None, None, None)

    return jax.shard_map(
        per_device,
        mesh=mesh,
        in_specs=(spec, P()),
        out_specs=(spec, spec),
        check_vma=False,
    )
```
